256 devices in a mesh: groups: 2 (over z), blk: 64 (over x, y), head: 2 (over core).
Axes of the slice: x: 8, y: 8, z: 2, core: 2. Of those that a mesh axis runs over, the one named last changes fastest.
The devices are a block of a 8x8x16 slice.
Arguments:
- q_latent: float32 [256, 128, 512], P(('groups', 'blk'), 'head'), parts along dimension 0, may hold values from -16 to 16
- q_rope: float32 [256, 128, 64], P(('groups', 'blk'), 'head'), parts along dimension 0, may hold values from -8 to 8
- cache_latent: float32 [262144, 512], P(('groups', 'blk')), parts along dimension 0, may hold values from -8 to 8
- cache_rope: float32 [262144, 64], P(('groups', 'blk')), parts along dimension 0, may hold values from -4 to 4
- home_offset: int32 [256], P(('groups', 'blk')), parts along dimension 0, may hold values from 0 to 14335
- lengths: int32 [256], P(('groups', 'blk')), parts along dimension 0, may hold values from 1 to 14336, as said below
Outputs:
- attended: float32 [256, 128, 512], P(('groups', 'blk'), 'head'), parts along dimension 0
The draws below stay inside these ranges and needn't reach their ends.
There are 2 independent parts, one for each index of `groups`. The reference program is written for one: setup_inputs(seed, part) draws one part's arguments, and reference() takes and returns one part's arrays. A program takes and returns all parts, laid end to end along the dimension named above; each array names one. Nothing has to cross between parts.
Inputs may be any that keep to these rules, and one draw needn't show every extreme that they name: `lengths`: some query has all 14336 cells live.
All inputs are finite; a program needn't handle non-finite values.
Results may differ from the reference program's by a relative error of at most 0.0003.
Values sent between devices are 32-bit elements; how exact they have to be, the bound alone decides.
No kernel may reach another device: no remote copies, remote signals or barrier semaphores. Data moves between devices by JAX's collectives and lax.ppermute only.
A program may use at most 64 MiB of HBM per device.

```python
import math
import jax
import jax.numpy as jnp
from jax import lax

LAT = 512
ROPE = 64
NOPE = 128
HEADS = 128
QDEV = 2
CACHE_DEV = 2048
HOPS = 3
BATCH = 128
SEQ = 131072
WINDOW = 14336


def layout(base_key):
    int_key = jax.random.fold_in(base_key, 7)
    beginnings = jax.random.randint(jax.random.fold_in(int_key, 1), (BATCH,), 0, WINDOW)
    extents = jax.random.randint(jax.random.fold_in(int_key, 2), (BATCH,), 1, WINDOW + 1)
    chosen = jax.random.randint(jax.random.fold_in(int_key, 3), (), 0, BATCH)
    query_ids = jnp.arange(BATCH)
    extents = jnp.where(query_ids == chosen, WINDOW, extents)
    return (beginnings.astype(jnp.int32), extents.astype(jnp.int32))


def tables(base_key):
    latent_key = jax.random.fold_in(base_key, 21)
    rotary_key = jax.random.fold_in(base_key, 22)
    latent = jax.random.truncated_normal(latent_key, -4.0, 4.0, (SEQ, LAT), jnp.float32)
    rotary = jax.random.truncated_normal(rotary_key, -4.0, 4.0, (SEQ, ROPE), jnp.float32)
    return (latent, rotary)


def draw_cache_latent(key, part):
    return tables(key)[0]


def draw_cache_rope(key, part):
    return tables(key)[1]


def draw_home_offset(key, part):
    return layout(key)[0]


def draw_lengths(key, part):
    return layout(key)[1]


def draw_q_latent(key, part):
    query_key = jax.random.fold_in(key, 31)
    queries = 2.0 * jax.random.truncated_normal(query_key, -4.0, 4.0, (BATCH, HEADS, LAT), jnp.float32)
    return queries


def draw_q_rope(key, part):
    query_key = jax.random.fold_in(key, 32)
    queries = 2.0 * jax.random.truncated_normal(query_key, -4.0, 4.0, (BATCH, HEADS, ROPE), jnp.float32)
    return queries


def setup_inputs(seed: int = 0, part: int = 0) -> dict:
    streams_of = jax.random.split(jax.random.key(seed), 7)
    part_keys = jax.random.split(jax.random.fold_in(streams_of[6], part), 7)
    q_latent = draw_q_latent(jax.random.fold_in(jax.random.fold_in(streams_of[6], part), 71), part)
    q_rope = draw_q_rope(jax.random.fold_in(jax.random.fold_in(streams_of[6], part), 71), part)
    cache_latent = draw_cache_latent(jax.random.fold_in(jax.random.fold_in(streams_of[6], part), 71), part)
    cache_rope = draw_cache_rope(jax.random.fold_in(jax.random.fold_in(streams_of[6], part), 71), part)
    home_offset = draw_home_offset(jax.random.fold_in(jax.random.fold_in(streams_of[6], part), 71), part)
    lengths = draw_lengths(jax.random.fold_in(jax.random.fold_in(streams_of[6], part), 71), part)
    return {"q_latent": q_latent, "q_rope": q_rope, "cache_latent": cache_latent, "cache_rope": cache_rope, "home_offset": home_offset, "lengths": lengths}


def reference(q_latent, q_rope, cache_latent, cache_rope, home_offset, lengths):
    scale = 1.0 / math.sqrt(NOPE + ROPE)
    offsets = jnp.arange(WINDOW, dtype=jnp.int32)

    def attend_one(packed):
        query, query_rope, index, beginning, extent = packed
        first_block = index // QDEV - HOPS
        positions = jnp.mod(first_block * CACHE_DEV + offsets, SEQ).astype(jnp.int32)
        keys = jnp.take(cache_latent, positions, axis=0)
        rope_keys = jnp.take(cache_rope, positions, axis=0)
        scores = (jnp.dot(query, keys.T, precision=lax.Precision.HIGHEST) + jnp.dot(query_rope, rope_keys.T, precision=lax.Precision.HIGHEST)) * scale
        validity = jnp.mod(offsets - beginning, WINDOW) < extent
        peak = lax.optimization_barrier(jnp.max(jnp.where(validity[None, :], scores, -jnp.inf), axis=1, keepdims=True))
        weights = jnp.where(validity[None, :], jnp.exp(scores - peak), 0.0)
        totals = lax.optimization_barrier(jnp.sum(weights, axis=1, keepdims=True))
        return jnp.dot(weights, keys, precision=lax.Precision.HIGHEST) / totals
    indices = jnp.arange(BATCH, dtype=jnp.int32)
    return lax.map(attend_one, (q_latent, q_rope, indices, home_offset, lengths))
```

```python
import functools
import math

import jax
import jax.numpy as jnp
from jax import lax
from jax.experimental import pallas as pl
from jax.experimental.pallas import tpu as pltpu
from jax.sharding import PartitionSpec as P

ROPE = 64
NOPE = 128
HOPS = 3
TILE = 512

SCALE = math.log2(math.e) / math.sqrt(NOPE + ROPE)
DEAD = -1e30
FLOOR = -1e29
MIB = 1024 * 1024
F32 = jnp.float32
BF16 = jnp.bfloat16

VMEM = pl.BlockSpec(memory_space=pltpu.VMEM)
SMEM = pl.BlockSpec(memory_space=pltpu.SMEM)


def call(body, outs, in_specs, args, flops, scratch=(), limit=24):
    nbytes = sum(math.prod(o.shape) * o.dtype.itemsize for o in outs)
    nbytes += sum(math.prod(a.shape) * a.dtype.itemsize for a in args)
    return pl.pallas_call(
        body,
        out_shape=outs,
        in_specs=in_specs,
        out_specs=[VMEM] * len(outs),
        scratch_shapes=list(scratch),
        compiler_params=pltpu.CompilerParams(vmem_limit_bytes=limit * MIB),
        cost_estimate=pl.CostEstimate(flops=flops, bytes_accessed=nbytes, transcendentals=0),
    )(*args)


def two_parts(x):
    high = x.astype(BF16)
    return high, (x - high.astype(F32)).astype(BF16)


def pack_body(home_ref, lengths_ref, latent_ref, rope_ref, out_ref):
    count, heads, width = latent_ref.shape
    rows = count * heads
    rope = rope_ref.shape[2]
    out_ref[0:width, :] = latent_ref[...].reshape(rows, width).T * SCALE
    flat = rope_ref[...].reshape(rows, rope)
    flat = jnp.concatenate([flat, jnp.zeros((rows, 128 - rope), F32)], axis=1)
    out_ref[width : width + rope, :] = flat.T[0:rope, :] * SCALE
    query = lax.broadcasted_iota(jnp.int32, (8, rows), 1) // heads
    which = lax.broadcasted_iota(jnp.int32, (8, rows), 0)
    home = jnp.zeros((8, rows), jnp.int32)
    extent = jnp.zeros((8, rows), jnp.int32)
    for q in range(count):
        home = jnp.where(query == q, home_ref[q], home)
        extent = jnp.where(query == q, lengths_ref[q], extent)
    out_ref[width + rope :, :] = jnp.where(which == 0, home, extent).astype(F32)


def pack(q_latent, q_rope, home_offset, lengths):
    count, heads, width = q_latent.shape
    rows = width + q_rope.shape[2] + 8
    out = [jax.ShapeDtypeStruct((rows, count * heads), F32)]
    return call(
        pack_body, out, [SMEM, SMEM, VMEM, VMEM], (home_offset, lengths, q_latent, q_rope), 1000
    )[0]


def prepare_body(latent_ref, rope_ref, ch_ref, cl_ref, th_ref, tl_ref, kr_ref):
    cells, width = latent_ref.shape
    rope = rope_ref.shape[0]

    def step(i, _):
        at = pl.ds(pl.multiple_of(i * 256, 256), 256)
        high, low = two_parts(latent_ref[at, :])
        ch_ref[at, :] = high
        cl_ref[at, :] = low
        th_ref[:, at] = high.T
        tl_ref[:, at] = low.T
        keys = jnp.concatenate([rope_ref[:, at], jnp.zeros((128 - rope, 256), F32)], axis=0).T
        high, low = two_parts(keys[:, 0:rope])
        kr_ref[at, :] = jnp.concatenate([high, low, high, low], axis=1)
        return 0

    lax.fori_loop(0, cells // 256, step, 0)


def prepare(cache_latent, cache_rope):
    cells, width = cache_latent.shape
    rope = cache_rope.shape[1]
    outs = [
        jax.ShapeDtypeStruct((cells, width), BF16),
        jax.ShapeDtypeStruct((cells, width), BF16),
        jax.ShapeDtypeStruct((width, cells), BF16),
        jax.ShapeDtypeStruct((width, cells), BF16),
        jax.ShapeDtypeStruct((cells, 4 * rope), BF16),
    ]
    return call(prepare_body, outs, [VMEM, VMEM], (cache_latent, cache_rope.T), 10**9, limit=32)


def attend_body(slots, *refs):
    n = len(slots)
    packs, rest = refs[:n], refs[n:]
    ch_ref, cl_ref, th_ref, tl_ref, kr_ref = rest[:5]
    outs, scores_ref = rest[5 : 5 + n], rest[5 + n]
    cells, width = ch_ref.shape
    rope = kr_ref.shape[1] // 4
    window = (2 * HOPS + 1) * cells
    rows = packs[0].shape[1]
    total_rows = n * rows

    def joined(lo, hi):
        return jnp.concatenate([p[lo:hi, :] for p in packs], axis=1)

    qh, ql = two_parts(joined(0, width))
    rh, rl = two_parts(joined(width, width + rope))
    qr = jnp.concatenate([rh, rh, rl, rl], axis=0)
    meta = joined(width + rope, width + rope + 8).astype(jnp.int32)
    first = meta[0:1, :] - jnp.concatenate(
        [jnp.full((1, rows), s * cells, jnp.int32) for s in slots], axis=1
    )
    extent = meta[1:2, :]

    def score(i, top):
        at = pl.ds(pl.multiple_of(i * TILE, TILE), TILE)
        high = ch_ref[at, :]
        s = (
            jnp.dot(high, qh, preferred_element_type=F32)
            + jnp.dot(high, ql, preferred_element_type=F32)
            + jnp.dot(cl_ref[at, :], qh, preferred_element_type=F32)
            + jnp.dot(kr_ref[at, :], qr, preferred_element_type=F32)
        )
        cell = lax.broadcasted_iota(jnp.int32, (TILE, total_rows), 0) + i * TILE
        offset = cell - first
        offset = jnp.where(offset < 0, offset + window, offset)
        s = jnp.where(offset < extent, s, DEAD)
        scores_ref[at, :] = s
        return jnp.maximum(top, jnp.max(s, axis=0, keepdims=True))

    start = jnp.full((1, total_rows), FLOOR, F32)
    peak = lax.fori_loop(0, cells // TILE, score, start)

    def weigh(i, carry):
        total, summed = carry
        at = pl.ds(pl.multiple_of(i * TILE, TILE), TILE)
        weights = jnp.exp2(scores_ref[at, :] - peak)
        total = total + jnp.sum(weights, axis=0, keepdims=True)
        wh, wl = two_parts(weights)
        product = (
            jnp.dot(th_ref[:, at], wh, preferred_element_type=F32)
            + jnp.dot(th_ref[:, at], wl, preferred_element_type=F32)
            + jnp.dot(tl_ref[:, at], wh, preferred_element_type=F32)
        )
        for k in range(n):
            outs[k][0:width, :] += product[:, k * rows : (k + 1) * rows]
        return total, summed

    for k in range(n):
        outs[k][0:width, :] = jnp.zeros((width, rows), F32)
    total, _ = lax.fori_loop(0, cells // TILE, weigh, (jnp.zeros((1, total_rows), F32), 0))
    for k in range(n):
        at = slice(k * rows, (k + 1) * rows)
        outs[k][width:, :] = jnp.concatenate(
            [peak[:, at], total[:, at], jnp.zeros((6, rows), F32)], axis=0
        )


def attend(packs, slots, prepared):
    n = len(packs)
    cells, width = prepared[0].shape
    rows = packs[0].shape[1]
    outs = [jax.ShapeDtypeStruct((width + 8, rows), F32)] * n
    return call(
        functools.partial(attend_body, tuple(slots)),
        outs,
        [VMEM] * (n + 5),
        tuple(packs) + tuple(prepared),
        2 * 6 * 128 * n * cells * 1088,
        scratch=[pltpu.VMEM((cells, n * rows), F32)],
    )


def merged(parts, width):
    peaks = [p[width : width + 1, :] for p in parts]
    peak = functools.reduce(jnp.maximum, peaks)
    scales = [jnp.exp2(x - peak) for x in peaks]
    total = sum(p[width + 1 : width + 2, :] * s for p, s in zip(parts, scales))
    summed = sum(p[0:width, :] * s for p, s in zip(parts, scales))
    return peak, total, summed


def merge_body(*refs):
    half = len(refs) // 3
    for k in range(half):
        a, b, out = refs[k], refs[half + k], refs[2 * half + k]
        width, rows = out.shape[0] - 8, out.shape[1]
        peak, total, summed = merged([a, b], width)
        out[0:width, :] = summed
        out[width:, :] = jnp.concatenate([peak, total, jnp.zeros((6, rows), F32)], axis=0)


def merge(left, right):
    outs = [jax.ShapeDtypeStruct(x.shape, F32) for x in left]
    args = tuple(left) + tuple(right)
    return call(merge_body, outs, [VMEM] * len(args), args, 10**6)


def finish_body(a_ref, b_ref, c_ref, out_ref):
    count, heads, width = out_ref.shape
    _, total, summed = merged([a_ref, b_ref, c_ref], width)
    out_ref[...] = (summed / total).T.reshape(count, heads, width)


def finish(own, upper, lower, shape):
    out = [jax.ShapeDtypeStruct(shape, F32)]
    return call(finish_body, out, [VMEM] * 3, (own, upper, lower), 10**6)[0]


def shift(x, by):
    size = lax.axis_size("blk")
    return lax.ppermute(x, "blk", [(i, (i + by) % size) for i in range(size)])


def shards(q_latent, q_rope, cache_latent, cache_rope, home_offset, lengths):
    own = pack(q_latent, q_rope, home_offset, lengths)
    up, down = shift(own, 1), shift(own, -1)
    prepared = prepare(cache_latent, cache_rope)
    here = attend([own], [HOPS], prepared)[0]
    partial = []
    for hop in range(1, HOPS + 1):
        held = (up, down)
        if hop < HOPS:
            up, down = shift(up, 1), shift(down, -1)
        partial.append(attend(held, [HOPS + hop, HOPS - hop], prepared))
    back = partial[-1]
    for hop in range(HOPS, 0, -1):
        back = [shift(back[0], -1), shift(back[1], 1)]
        if hop > 1:
            back = merge(back, partial[hop - 2])
    return finish(here, back[0], back[1], q_latent.shape)


def solution(mesh):
    return jax.shard_map(
        shards,
        mesh=mesh,
        in_specs=(
            P(("groups", "blk"), "head", None),
            P(("groups", "blk"), "head", None),
            P(("groups", "blk"), None),
            P(("groups", "blk"), None),
            P(("groups", "blk")),
            P(("groups", "blk")),
        ),
        out_specs=P(("groups", "blk"), "head", None),
        check_vma=False,
    )
```

```python
import functools
import math

import jax
import jax.numpy as jnp
from jax import lax
from jax.experimental import pallas as pl
from jax.experimental.pallas import tpu as pltpu
from jax.sharding import PartitionSpec as P


ROPE = 64
NOPE = 128
HOPS = 3
TILE = 1024

SCALE = math.log2(math.e) / math.sqrt(NOPE + ROPE)
DEAD = -1e30
FLOOR = -1e29
MIB = 1024 * 1024
F32 = jnp.float32
BF16 = jnp.bfloat16

VMEM = pl.BlockSpec(memory_space=pltpu.VMEM)
HBM = pl.BlockSpec(memory_space=pltpu.HBM)


def call(body, outs, in_specs, args, flops, scratch=(), limit=24):
    nbytes = sum(math.prod(o.shape) * o.dtype.itemsize for o in outs)
    nbytes += sum(math.prod(a.shape) * a.dtype.itemsize for a in args)
    return pl.pallas_call(
        body,
        out_shape=outs,
        in_specs=in_specs,
        out_specs=[VMEM] * len(outs),
        scratch_shapes=list(scratch),
        compiler_params=pltpu.CompilerParams(vmem_limit_bytes=limit * MIB),
        cost_estimate=pl.CostEstimate(flops=flops, bytes_accessed=nbytes, transcendentals=0),
    )(*args)


def dot(a, b):
    return jnp.dot(a, b, preferred_element_type=F32)


def two_parts(x):
    high = x.astype(BF16)
    return high, (x - high.astype(F32)).astype(BF16)


def pack_body(home_hbm, lengths_hbm, latent_hbm, rope_hbm, out_ref, home_ref, lengths_ref, latent_ref, rope_ref, sems):
    moves = [
        pltpu.make_async_copy(src, dst, sems.at[k])
        for k, (src, dst) in enumerate(
            [
                (latent_hbm, latent_ref),
                (rope_hbm, rope_ref),
                (home_hbm, home_ref),
                (lengths_hbm, lengths_ref),
            ]
        )
    ]
    for move in moves:
        move.start()
    for move in moves:
        move.wait()
    count, heads, width = latent_ref.shape
    rows = count * heads
    rope = rope_ref.shape[2]
    out_ref[0:width, :] = latent_ref[...].reshape(rows, width).T * SCALE
    flat = rope_ref[...].reshape(rows, rope)
    flat = jnp.concatenate([flat, jnp.zeros((rows, 128 - rope), F32)], axis=1)
    out_ref[width : width + rope, :] = flat.T[0:rope, :] * SCALE
    query = lax.broadcasted_iota(jnp.int32, (8, rows), 1) // heads
    which = lax.broadcasted_iota(jnp.int32, (8, rows), 0)
    home = jnp.zeros((8, rows), jnp.int32)
    extent = jnp.zeros((8, rows), jnp.int32)
    for q in range(count):
        home = jnp.where(query == q, home_ref[q], home)
        extent = jnp.where(query == q, lengths_ref[q], extent)
    out_ref[width + rope :, :] = jnp.where(which == 0, home, extent).astype(F32)


def pack(q_latent, q_rope, home_offset, lengths):
    count, heads, width = q_latent.shape
    rows = width + q_rope.shape[2] + 8
    out = [jax.ShapeDtypeStruct((rows, count * heads), F32)]
    scratch = [
        pltpu.SMEM(home_offset.shape, jnp.int32),
        pltpu.SMEM(lengths.shape, jnp.int32),
        pltpu.VMEM(q_latent.shape, F32),
        pltpu.VMEM(q_rope.shape, F32),
        pltpu.SemaphoreType.DMA((4,)),
    ]
    args = (home_offset, lengths, q_latent, q_rope)
    return call(pack_body, out, [HBM] * 4, args, 1000, scratch, limit=57)[0]


def prepare_body(latent_hbm, rope_hbm, ch_ref, cl_ref, th_ref, tl_ref, kr_ref, latent_ref, rope_ref, sems):
    cells = latent_hbm.shape[0]
    rope = rope_hbm.shape[0]
    piece = 256
    moves = [pltpu.make_async_copy(rope_hbm, rope_ref, sems.at[cells // piece])]
    for i in range(cells // piece):
        at = pl.ds(i * piece, piece)
        moves.append(pltpu.make_async_copy(latent_hbm.at[at], latent_ref.at[at], sems.at[i]))
    for move in moves:
        move.start()
    moves[0].wait()
    for i in range(cells // piece):
        at = slice(i * piece, (i + 1) * piece)
        moves[i + 1].wait()
        high, low = two_parts(latent_ref[at, :])
        ch_ref[at, :] = high
        cl_ref[at, :] = low
        th_ref[:, at] = high.T
        tl_ref[:, at] = low.T
        keys = jnp.concatenate([rope_ref[:, at], jnp.zeros((128 - rope, piece), F32)], axis=0).T
        high, low = two_parts(keys[:, 0:rope])
        kr_ref[at, :] = jnp.concatenate([high, low, high, low], axis=1)


def prepare(cache_latent, cache_rope):
    cells, width = cache_latent.shape
    rope = cache_rope.shape[1]
    outs = [
        jax.ShapeDtypeStruct((cells, width), BF16),
        jax.ShapeDtypeStruct((cells, width), BF16),
        jax.ShapeDtypeStruct((width, cells), BF16),
        jax.ShapeDtypeStruct((width, cells), BF16),
        jax.ShapeDtypeStruct((cells, 4 * rope), BF16),
    ]
    scratch = [
        pltpu.VMEM(cache_latent.shape, F32),
        pltpu.VMEM((rope, cells), F32),
        pltpu.SemaphoreType.DMA((cells // 256 + 1,)),
    ]
    args = (cache_latent, cache_rope.T)
    return call(prepare_body, outs, [HBM] * 2, args, 10**9, scratch, limit=44)


def attend_body(hop, sides, *refs):
    n = len(sides)
    packs, rest = refs[:n], refs[n:]
    ch_ref, cl_ref, th_ref, tl_ref, kr_ref = rest[:5]
    outs, scores_ref = rest[5 : 5 + n], rest[5 + n]
    cells, width = ch_ref.shape
    rope = kr_ref.shape[1] // 4
    window = (2 * HOPS + 1) * cells
    rows = packs[0].shape[1]
    total_rows = n * rows

    def joined(lo, hi):
        return jnp.concatenate([p[lo:hi, :] for p in packs], axis=1)

    def times_both(left, high, low):
        if n > 1:
            return dot(left, high) + dot(left, low)
        both = dot(left, jnp.concatenate([high, low], axis=1))
        return both[:, :total_rows] + both[:, total_rows:]

    qh, ql = two_parts(joined(0, width))
    rh, rl = two_parts(joined(width, width + rope))
    qr = jnp.concatenate([rh, rh, rl, rl], axis=0)
    meta = joined(width + rope, width + rope + 8).astype(jnp.int32)
    place = 1 - 2 * lax.rem(lax.axis_index("blk"), 2)
    slots = [HOPS - hop * place * side for side in sides]
    first = meta[0:1, :] - jnp.concatenate(
        [jnp.full((1, rows), s * cells, jnp.int32) for s in slots], axis=1
    )
    extent = meta[1:2, :]

    def score(i, top):
        at = pl.ds(pl.multiple_of(i * TILE, TILE), TILE)
        s = (
            times_both(ch_ref[at, :], qh, ql)
            + dot(cl_ref[at, :], qh)
            + dot(kr_ref[at, :], qr)
        )
        cell = lax.broadcasted_iota(jnp.int32, (TILE, total_rows), 0) + i * TILE
        offset = cell - first
        offset = jnp.where(offset < 0, offset + window, offset)
        s = jnp.where(offset < extent, s, DEAD)
        scores_ref[at, :] = s
        return jnp.maximum(top, jnp.max(s, axis=0, keepdims=True))

    start = jnp.full((1, total_rows), FLOOR, F32)
    peak = lax.fori_loop(0, cells // TILE, score, start)

    def weigh(i, total):
        at = pl.ds(pl.multiple_of(i * TILE, TILE), TILE)
        weights = jnp.exp2(scores_ref[at, :] - peak)
        wh, wl = two_parts(weights)
        product = times_both(th_ref[:, at], wh, wl) + dot(tl_ref[:, at], wh)
        for k in range(n):
            outs[k][0:width, :] += product[:, k * rows : (k + 1) * rows]
        return total + jnp.sum(weights, axis=0, keepdims=True)

    for k in range(n):
        outs[k][0:width, :] = jnp.zeros((width, rows), F32)
    total = lax.fori_loop(0, cells // TILE, weigh, jnp.zeros((1, total_rows), F32))
    for k in range(n):
        at = slice(k * rows, (k + 1) * rows)
        outs[k][width:, :] = jnp.concatenate(
            [peak[:, at], total[:, at], jnp.zeros((6, rows), F32)], axis=0
        )


def attend(packs, hop, sides, prepared):
    n = len(packs)
    cells, width = prepared[0].shape
    rows = packs[0].shape[1]
    outs = [jax.ShapeDtypeStruct((width + 8, rows), F32)] * n
    return call(
        functools.partial(attend_body, hop, sides),
        outs,
        [VMEM] * (n + 5),
        tuple(packs) + tuple(prepared),
        2 * 6 * 128 * n * cells * 1088,
        scratch=[pltpu.VMEM((cells, n * rows), F32)],
    )


def merged(parts, width):
    peaks = [p[width : width + 1, :] for p in parts]
    peak = functools.reduce(jnp.maximum, peaks)
    scales = [jnp.exp2(x - peak) for x in peaks]
    total = sum(p[width + 1 : width + 2, :] * s for p, s in zip(parts, scales))
    summed = sum(p[0:width, :] * s for p, s in zip(parts, scales))
    return peak, total, summed


def merge_body(a, b, out):
    width, rows = out.shape[0] - 8, out.shape[1]
    peak, total, summed = merged([a, b], width)
    out[0:width, :] = summed
    out[width:, :] = jnp.concatenate([peak, total, jnp.zeros((6, rows), F32)], axis=0)


def merge(left, right):
    outs = [jax.ShapeDtypeStruct(left.shape, F32)]
    return call(merge_body, outs, [VMEM] * 2, (left, right), 10**6)[0]


def finish_body(a_ref, b_ref, c_ref, out_ref):
    count, heads, width = out_ref.shape
    _, total, summed = merged([a_ref, b_ref, c_ref], width)
    out_ref[...] = (summed / total).T.reshape(count, heads, width)


def finish(own, upper, lower, shape):
    out = [jax.ShapeDtypeStruct(shape, F32)]
    return call(finish_body, out, [VMEM] * 3, (own, upper, lower), 10**6)[0]


def swap(x, parity):
    size = lax.axis_size("blk")
    pairs = []
    for i in range(parity, size + parity, 2):
        pairs += [(i % size, (i + 1) % size), ((i + 1) % size, i % size)]
    return lax.ppermute(x, "blk", pairs)


def shards(q_latent, q_rope, cache_latent, cache_rope, home_offset, lengths):
    own = pack(q_latent, q_rope, home_offset, lengths)
    even, odd = swap(own, 0), swap(own, 1)
    prepared = prepare(cache_latent, cache_rope)
    evens, odds = [even], [odd]
    for _ in range(2, HOPS + 1):
        even, odd = (swap(odds[-1], 0), swap(evens[-1], 1))
        evens.append(even)
        odds.append(odd)
    partial = [
        attend([evens[hop - 1], odds[hop - 1]], hop, (1, -1), prepared)
        for hop in range(1, HOPS)
    ]
    even = attend([even], HOPS, (1,), prepared)[0]
    odd = attend([odd], HOPS, (-1,), prepared)[0]
    here = attend([own], 0, (1,), prepared)[0]
    for hop in range(HOPS, 0, -1):
        even, odd = swap(even, 0), swap(odd, 1)
        if hop > 1:
            even, odd = merge(odd, partial[hop - 2][0]), merge(even, partial[hop - 2][1])
    return finish(here, even, odd, q_latent.shape)


def solution(mesh):
    return jax.shard_map(
        shards,
        mesh=mesh,
        in_specs=(
            P(("groups", "blk"), "head", None),
            P(("groups", "blk"), "head", None),
            P(("groups", "blk"), None),
            P(("groups", "blk"), None),
            P(("groups", "blk")),
            P(("groups", "blk")),
        ),
        out_specs=P(("groups", "blk"), "head", None),
        check_vma=False,
    )
```

```python
import functools
import math

import jax
import jax.numpy as jnp
from jax import lax
from jax.experimental import pallas as pl
from jax.experimental.pallas import tpu as pltpu
from jax.sharding import PartitionSpec as P


ROPE = 64
NOPE = 128
HOPS = 3
TILE = 1024

SCALE = math.log2(math.e) / math.sqrt(NOPE + ROPE)
DEAD = -1e30
FLOOR = -1e29
MIB = 1024 * 1024
F32 = jnp.float32
BF16 = jnp.bfloat16

VMEM = pl.BlockSpec(memory_space=pltpu.VMEM)
ANY = pl.BlockSpec(memory_space=pl.ANY)


def call(body, outs, in_specs, args, flops, scratch=(), limit=24):
    nbytes = sum(math.prod(o.shape) * o.dtype.itemsize for o in outs)
    nbytes += sum(math.prod(a.shape) * a.dtype.itemsize for a in args)
    return pl.pallas_call(
        body,
        out_shape=outs,
        in_specs=in_specs,
        out_specs=[VMEM] * len(outs),
        scratch_shapes=list(scratch),
        compiler_params=pltpu.CompilerParams(vmem_limit_bytes=limit * MIB),
        cost_estimate=pl.CostEstimate(flops=flops, bytes_accessed=nbytes, transcendentals=0),
    )(*args)


def in_hbm(x):
    return pltpu.with_memory_space_constraint(x, pltpu.HBM)


def dot(a, b):
    return jnp.dot(a, b, preferred_element_type=F32)


def two_parts(x):
    high = x.astype(BF16)
    return high, (x - high.astype(F32)).astype(BF16)


def pack_body(home_hbm, lengths_hbm, latent_hbm, rope_hbm, out_ref, home_ref, lengths_ref, latent_ref, rope_ref, sems):
    moves = [
        pltpu.make_async_copy(src, dst, sems.at[k])
        for k, (src, dst) in enumerate(
            [
                (latent_hbm, latent_ref),
                (rope_hbm, rope_ref),
                (home_hbm, home_ref),
                (lengths_hbm, lengths_ref),
            ]
        )
    ]
    for move in moves:
        move.start()
    for move in moves:
        move.wait()
    count, heads, width = latent_ref.shape
    rows = count * heads
    rope = rope_ref.shape[2]
    out_ref[0:width, :] = latent_ref[...].reshape(rows, width).T * SCALE
    flat = rope_ref[...].reshape(rows, rope)
    flat = jnp.concatenate([flat, jnp.zeros((rows, 128 - rope), F32)], axis=1)
    out_ref[width : width + rope, :] = flat.T[0:rope, :] * SCALE
    query = lax.broadcasted_iota(jnp.int32, (8, rows), 1) // heads
    which = lax.broadcasted_iota(jnp.int32, (8, rows), 0)
    home = jnp.zeros((8, rows), jnp.int32)
    extent = jnp.zeros((8, rows), jnp.int32)
    for q in range(count):
        home = jnp.where(query == q, home_ref[q], home)
        extent = jnp.where(query == q, lengths_ref[q], extent)
    out_ref[width + rope :, :] = jnp.where(which == 0, home, extent).astype(F32)


def pack(q_latent, q_rope, home_offset, lengths):
    count, heads, width = q_latent.shape
    rows = width + q_rope.shape[2] + 8
    out = [jax.ShapeDtypeStruct((rows, count * heads), F32)]
    scratch = [
        pltpu.SMEM(home_offset.shape, jnp.int32),
        pltpu.SMEM(lengths.shape, jnp.int32),
        pltpu.VMEM(q_latent.shape, F32),
        pltpu.VMEM(q_rope.shape, F32),
        pltpu.SemaphoreType.DMA((4,)),
    ]
    args = tuple(in_hbm(x) for x in (home_offset, lengths, q_latent, q_rope))
    return call(pack_body, out, [ANY] * 4, args, 1000, scratch)[0]


def prepare_body(latent_hbm, rope_hbm, ch_ref, cl_ref, th_ref, tl_ref, kr_ref, latent_ref, rope_ref, sems):
    cells = latent_hbm.shape[0]
    rope = rope_hbm.shape[0]
    piece = 256
    moves = [pltpu.make_async_copy(rope_hbm, rope_ref, sems.at[cells // piece])]
    for i in range(cells // piece):
        at = pl.ds(i * piece, piece)
        moves.append(pltpu.make_async_copy(latent_hbm.at[at], latent_ref.at[at], sems.at[i]))
    for move in moves:
        move.start()
    moves[0].wait()
    for i in range(cells // piece):
        at = slice(i * piece, (i + 1) * piece)
        moves[i + 1].wait()
        high, low = two_parts(latent_ref[at, :])
        ch_ref[at, :] = high
        cl_ref[at, :] = low
        th_ref[:, at] = high.T
        tl_ref[:, at] = low.T
        keys = jnp.concatenate([rope_ref[:, at], jnp.zeros((128 - rope, piece), F32)], axis=0).T
        high, low = two_parts(keys[:, 0:rope])
        kr_ref[at, :] = jnp.concatenate([high, low, high, low], axis=1)


def prepare(cache_latent, cache_rope):
    cells, width = cache_latent.shape
    rope = cache_rope.shape[1]
    outs = [
        jax.ShapeDtypeStruct((cells, width), BF16),
        jax.ShapeDtypeStruct((cells, width), BF16),
        jax.ShapeDtypeStruct((width, cells), BF16),
        jax.ShapeDtypeStruct((width, cells), BF16),
        jax.ShapeDtypeStruct((cells, 4 * rope), BF16),
    ]
    scratch = [
        pltpu.VMEM(cache_latent.shape, F32),
        pltpu.VMEM((rope, cells), F32),
        pltpu.SemaphoreType.DMA((cells // 256 + 1,)),
    ]
    args = (in_hbm(cache_latent), in_hbm(cache_rope.T))
    return call(prepare_body, outs, [ANY] * 2, args, 10**9, scratch)


def attend_body(hop, sides, *refs):
    n = len(sides)
    packs, rest = refs[:n], refs[n:]
    ch_ref, cl_ref, th_ref, tl_ref, kr_ref = rest[:5]
    outs, scores_ref = rest[5 : 5 + n], rest[5 + n]
    cells, width = ch_ref.shape
    rope = kr_ref.shape[1] // 4
    window = (2 * HOPS + 1) * cells
    rows = packs[0].shape[1]
    total_rows = n * rows

    def joined(lo, hi):
        return jnp.concatenate([p[lo:hi, :] for p in packs], axis=1)

    def times_both(left, high, low):
        if n > 1:
            return dot(left, high) + dot(left, low)
        both = dot(left, jnp.concatenate([high, low], axis=1))
        return both[:, :total_rows] + both[:, total_rows:]

    qh, ql = two_parts(joined(0, width))
    rh, rl = two_parts(joined(width, width + rope))
    qr = jnp.concatenate([rh, rh, rl, rl], axis=0)
    meta = joined(width + rope, width + rope + 8).astype(jnp.int32)
    place = 1 - 2 * lax.rem(lax.axis_index("blk"), 2)
    slots = [HOPS - hop * place * side for side in sides]
    first = meta[0:1, :] - jnp.concatenate(
        [jnp.full((1, rows), s * cells, jnp.int32) for s in slots], axis=1
    )
    extent = meta[1:2, :]

    def score(i, top):
        at = pl.ds(pl.multiple_of(i * TILE, TILE), TILE)
        s = (
            times_both(ch_ref[at, :], qh, ql)
            + dot(cl_ref[at, :], qh)
            + dot(kr_ref[at, :], qr)
        )
        cell = lax.broadcasted_iota(jnp.int32, (TILE, total_rows), 0) + i * TILE
        offset = cell - first
        offset = jnp.where(offset < 0, offset + window, offset)
        s = jnp.where(offset < extent, s, DEAD)
        scores_ref[at, :] = s
        return jnp.maximum(top, jnp.max(s, axis=0, keepdims=True))

    start = jnp.full((1, total_rows), FLOOR, F32)
    peak = lax.fori_loop(0, cells // TILE, score, start)

    def weigh(i, total):
        at = pl.ds(pl.multiple_of(i * TILE, TILE), TILE)
        weights = jnp.exp2(scores_ref[at, :] - peak)
        wh, wl = two_parts(weights)
        product = times_both(th_ref[:, at], wh, wl) + dot(tl_ref[:, at], wh)
        for k in range(n):
            outs[k][0:width, :] += product[:, k * rows : (k + 1) * rows]
        return total + jnp.sum(weights, axis=0, keepdims=True)

    for k in range(n):
        outs[k][0:width, :] = jnp.zeros((width, rows), F32)
    total = lax.fori_loop(0, cells // TILE, weigh, jnp.zeros((1, total_rows), F32))
    for k in range(n):
        at = slice(k * rows, (k + 1) * rows)
        outs[k][width:, :] = jnp.concatenate(
            [peak[:, at], total[:, at], jnp.zeros((6, rows), F32)], axis=0
        )


def attend(packs, hop, sides, prepared):
    n = len(packs)
    cells, width = prepared[0].shape
    rows = packs[0].shape[1]
    outs = [jax.ShapeDtypeStruct((width + 8, rows), F32)] * n
    return call(
        functools.partial(attend_body, hop, sides),
        outs,
        [VMEM] * (n + 5),
        tuple(packs) + tuple(prepared),
        2 * 6 * 128 * n * cells * 1088,
        scratch=[pltpu.VMEM((cells, n * rows), F32)],
    )


def merged(parts, width):
    peaks = [p[width : width + 1, :] for p in parts]
    peak = functools.reduce(jnp.maximum, peaks)
    scales = [jnp.exp2(x - peak) for x in peaks]
    total = sum(p[width + 1 : width + 2, :] * s for p, s in zip(parts, scales))
    summed = sum(p[0:width, :] * s for p, s in zip(parts, scales))
    return peak, total, summed


def merge_body(a, b, out):
    width, rows = out.shape[0] - 8, out.shape[1]
    peak, total, summed = merged([a, b], width)
    out[0:width, :] = summed
    out[width:, :] = jnp.concatenate([peak, total, jnp.zeros((6, rows), F32)], axis=0)


def merge(left, right):
    outs = [jax.ShapeDtypeStruct(left.shape, F32)]
    return call(merge_body, outs, [VMEM] * 2, (left, right), 10**6)[0]


def finish_body(a_ref, b_ref, c_ref, out_ref):
    count, heads, width = out_ref.shape
    _, total, summed = merged([a_ref, b_ref, c_ref], width)
    out_ref[...] = (summed / total).T.reshape(count, heads, width)


def finish(own, upper, lower, shape):
    out = [jax.ShapeDtypeStruct(shape, F32)]
    return call(finish_body, out, [VMEM] * 3, (own, upper, lower), 10**6)[0]


def swap(x, parity):
    size, cores = lax.axis_size("blk"), lax.axis_size("head")
    pairs = []
    for core in range(cores):
        for i in range(parity, size + parity, 2):
            one, two = i % size * cores + core, (i + 1) % size * cores + core
            pairs += [(one, two), (two, one)]
    return lax.ppermute(x, ("blk", "head"), pairs)


def shards(q_latent, q_rope, cache_latent, cache_rope, home_offset, lengths):
    own = pack(q_latent, q_rope, home_offset, lengths)
    even, odd = swap(own, 0), swap(own, 1)
    prepared = prepare(cache_latent, cache_rope)
    evens, odds = [even], [odd]
    for _ in range(2, HOPS + 1):
        even, odd = (swap(odds[-1], 0), swap(evens[-1], 1))
        evens.append(even)
        odds.append(odd)
    partial = [
        attend([evens[hop - 1], odds[hop - 1]], hop, (1, -1), prepared)
        for hop in range(1, HOPS)
    ]
    even = attend([even], HOPS, (1,), prepared)[0]
    odd = attend([odd], HOPS, (-1,), prepared)[0]
    here = attend([own], 0, (1,), prepared)[0]
    for hop in range(HOPS, 0, -1):
        even, odd = swap(even, 0), swap(odd, 1)
        if hop > 1:
            even, odd = merge(odd, partial[hop - 2][0]), merge(even, partial[hop - 2][1])
    return finish(here, even, odd, q_latent.shape)


def solution(mesh):
    return jax.shard_map(
        shards,
        mesh=mesh,
        in_specs=(
            P(("groups", "blk"), "head", None),
            P(("groups", "blk"), "head", None),
            P(("groups", "blk"), None),
            P(("groups", "blk"), None),
            P(("groups", "blk")),
            P(("groups", "blk")),
        ),
        out_specs=P(("groups", "blk"), "head", None),
        check_vma=False,
    )
```
